32 devices in a mesh: macro: 8 (over z, x), rep: 4 (over y, core).
Axes of the slice: x: 2, y: 2, z: 4, core: 2. Of those that a mesh axis runs over, the one named last changes fastest.
Arguments:
- u_old: float32 [4096], P('macro'), may hold values from -1 to 1
- coarse_kinetic_speed: float32 [4096], P('macro'), may hold values from 0.2 to 3
- micro_spreading_coefficient: float32 [4096], P('macro'), may hold values from 0.08 to 0.4
- micro_seed: int32 [4, 4096, 256], P('rep', 'macro'), may hold values from 0 to 1073741823
Outputs:
- new_state: float32 [4096], P('macro')
The draws below stay inside these ranges and needn't reach their ends.
All inputs are finite; a program needn't handle non-finite values.
Results may differ from the reference program's by a relative error of at most 0.0001.
Values sent between devices are 32-bit elements; how exact they have to be, the bound alone decides.
A program may use at most 64 MiB of HBM per device.

```python
import math
import jax
import jax.numpy as jnp
from jax import lax

CELLS = 256
STEPS = 8
ITERS = 4
REPS = 4
NMAC = 4096


def draw_coarse_kinetic_speed(key, part):
    place = jnp.arange(NMAC).astype(jnp.float32) / max(NMAC - 1, 1)
    base = jnp.exp(jax.random.uniform(key, (NMAC,), jnp.float32, jnp.log(0.2), jnp.log(0.3)))
    ramp = jnp.exp(jnp.log(10.0) * place)
    return jnp.clip(base * ramp, 0.2, 3.0)


def draw_u_old(key, part):
    place = jnp.arange(NMAC).astype(jnp.float32) / max(NMAC - 1, 1)
    rough = jax.random.uniform(jax.random.fold_in(key, 17), (NMAC,), jnp.float32, -1.0, 1.0)
    envelope = jnp.exp(jnp.log(0.1) * (1.0 - place))
    values = envelope * rough
    return jnp.clip(values, -1.0, 1.0)


def place_ends(values, key, low, largest):
    dims = values.shape
    spot = [jax.random.randint(jax.random.fold_in(key, axis), (), 0, dims[axis]) for axis in range(len(dims))]
    values = values.at[tuple(spot)].set(low)
    longest = dims.index(max(dims))
    spot[longest] = (spot[longest] + 1) % dims[longest]
    return values.at[tuple(spot)].set(largest)


def block_levels(key, extent, split, least, high):
    loudness, own = 1.0, jax.random.fold_in(key, 6)
    for dim, parts in split:
        heights = jnp.exp(jax.random.uniform(jax.random.fold_in(own, dim), (parts,), jnp.float32, least / len(split), high / len(split)))
        loudness = loudness * jnp.repeat(heights, extent[dim] // parts).reshape([-1 if axis == dim else 1 for axis in range(len(extent))])
    return loudness


def setup_inputs(seed: int = 0) -> dict:
    arg_keys = jax.random.split(jax.random.key(seed), 5)
    return {
        "u_old": draw_u_old(jax.random.fold_in(arg_keys[4], 71), 0),
        "coarse_kinetic_speed": draw_coarse_kinetic_speed(jax.random.fold_in(arg_keys[4], 71), 0),
        "micro_spreading_coefficient": jnp.clip(jnp.exp(math.log(0.4) - 1.609438 * jax.random.uniform(arg_keys[2], (NMAC,), jnp.float32) ** block_levels(arg_keys[2], (NMAC,), ((0, 8),), -0.2, 0.2)), 0.08, 0.4),
        "micro_seed": place_ends(jax.random.randint(arg_keys[3], (REPS, NMAC, CELLS), 0, 1073741824), jax.random.fold_in(arg_keys[3], 1), 0, 1073741823).astype(jnp.int32),
    }


noise_amp = 1.0
micro_dt = 0.02
proj_step = 0.25
fd_step = 0.01
seed_scale = 2.0 ** (-30)

def lifted(padded_density, cells):
    left = padded_density[:-2]
    centre = padded_density[1:-1]
    right = padded_density[2:]
    slope = 0.5 * (right - left)
    bend = 0.5 * (right - 2.0 * centre + left)
    place = (jnp.arange(cells).astype(jnp.float32) + 0.5) / cells - 0.5
    inside = centre[:, None] + slope[:, None] * place[None, :] + bend[:, None] * (place * place)[None, :]
    edge = 0.5 + 0.5 / cells
    ghost_left = centre - slope * edge + bend * edge * edge
    ghost_right = centre + slope * edge + bend * edge * edge
    return (inside, ghost_left, ghost_right)

def ensemble_aggregate(padded_density, pointwise_kinetic_speed, spreading_current, stochastic_kick):
    inside, ghost_left, ghost_right = lifted(padded_density, stochastic_kick.shape[2])
    start = inside[None] + stochastic_kick
    count = stochastic_kick.shape[0]
    left_col = jnp.broadcast_to(ghost_left[None, :, None], (count, ghost_left.shape[0], 1))
    right_col = jnp.broadcast_to(ghost_right[None, :, None], (count, ghost_right.shape[0], 1))
    kappa = spreading_current[None, :, None]
    growth = micro_dt * pointwise_kinetic_speed[None, :, None]
    state = start
    for step in range(STEPS):
        upper = jnp.concatenate([state[:, :, 1:], right_col], axis=2)
        lower = jnp.concatenate([left_col, state[:, :, :-1]], axis=2)
        state = state + kappa * (upper + lower - 2.0 * state) + growth * (state - state * state * state)
    return lax.optimization_barrier(jnp.sum(state - start, axis=(0, 2)))

def least_squares(hess, beta, iters):
    target = [beta] + [beta * 0.0 for index in range(iters)]
    cosines = []
    sines = []
    upper = []
    for col_index in range(iters):
        column = [hess[row][col_index] for row in range(col_index + 2)]
        for row in range(col_index):
            first = column[row]
            second = column[row + 1]
            column[row] = cosines[row] * first + sines[row] * second
            column[row + 1] = -sines[row] * first + cosines[row] * second
        radius = jnp.sqrt(column[col_index] * column[col_index] + column[col_index + 1] * column[col_index + 1])
        cosine = column[col_index] / radius
        sine = column[col_index + 1] / radius
        cosines.append(cosine)
        sines.append(sine)
        column[col_index] = radius
        upper.append(column[:col_index + 1])
        head = target[col_index]
        target[col_index] = cosine * head
        target[col_index + 1] = -sine * head
    solved = [None] * iters
    for row in range(iters - 1, -1, -1):
        acc = target[row]
        for later in range(row + 1, iters):
            acc = acc - upper[later][row] * solved[later]
        solved[row] = acc / upper[row][row]
    return solved

def reference(u_old, coarse_kinetic_speed, micro_spreading_coefficient, micro_seed):
    stochastic_kick = noise_amp * (micro_seed.astype(jnp.float32) * seed_scale - 0.5)
    fluctuation_amplitude = 1.0 / (REPS * CELLS * STEPS * micro_dt)

    def drift(species_density):
        return ensemble_aggregate(jnp.pad(species_density, 1), coarse_kinetic_speed, micro_spreading_coefficient, stochastic_kick) * fluctuation_amplitude
    f_old = drift(u_old)
    u_start = u_old + proj_step * f_old
    f_start = drift(u_start)
    resid = -(u_start - u_old - proj_step * f_start)
    delta = fd_step * math.sqrt(NMAC)
    beta = jnp.sqrt(jnp.sum(resid * resid))
    basis = [resid / beta]
    hess = [[None] * ITERS for row in range(ITERS + 1)]
    for col_index in range(ITERS):
        probe = basis[col_index]
        image = probe - proj_step * (drift(u_start + delta * probe) - f_start) / delta
        for row in range(col_index + 1):
            coeff = jnp.sum(basis[row] * image)
            hess[row][col_index] = coeff
            image = image - coeff * basis[row]
        length = jnp.sqrt(jnp.sum(image * image))
        hess[col_index + 1][col_index] = length
        basis.append(image / length)
    coeffs = least_squares(hess, beta, ITERS)
    result = u_start
    for col_index in range(ITERS):
        result = result + coeffs[col_index] * basis[col_index]
    return result
```

```python
import functools
import math

import jax
import jax.numpy as jnp
from jax import lax
from jax.experimental import pallas as pl
from jax.experimental.pallas import tpu as pltpu
from jax.sharding import PartitionSpec as P

STEPS = 8
ITERS = 4
LANES = 128
SUB = 8

noise_amp = 1.0
micro_dt = 0.02
proj_step = 0.25
fd_step = 0.01
seed_scale = 2.0 ** (-30)

MESH = pl.DeviceIdType.MESH


def total(values):
    return jnp.sum(jnp.sum(values, axis=0, keepdims=True), axis=1, keepdims=True)


class Givens:
    def __init__(self, beta):
        self.target = [beta]
        self.cosines = []
        self.sines = []
        self.upper = []

    def add(self, column):
        column = list(column)
        last = len(column) - 2
        for row in range(last):
            first, second = column[row], column[row + 1]
            column[row] = self.cosines[row] * first + self.sines[row] * second
            column[row + 1] = -self.sines[row] * first + self.cosines[row] * second
        radius = jnp.sqrt(column[last] * column[last] + column[last + 1] * column[last + 1])
        cosine = column[last] / radius
        sine = column[last + 1] / radius
        self.cosines.append(cosine)
        self.sines.append(sine)
        column[last] = radius
        self.upper.append(column[: last + 1])
        head = self.target[last]
        self.target[last] = cosine * head
        self.target.append(-sine * head)

    def solve(self):
        count = len(self.upper)
        solved = [None] * count
        for row in range(count - 1, -1, -1):
            acc = self.target[row]
            for later in range(row + 1, count):
                acc = acc - self.upper[later][row] * solved[later]
            solved[row] = acc / self.upper[row][row]
        return solved


def kernel(
    macros,
    reps,
    cells,
    rows,
    u_ref,
    rate_ref,
    kappa_ref,
    seed_ref,
    out_ref,
    raw,
    flipped,
    noise,
    noise_sum,
    coefs,
    parts,
    whole,
    load_sem,
    part_send,
    part_recv,
    whole_send,
    whole_recv,
):
    depth = cells // SUB
    pitch = flipped.shape[0] // SUB
    me = lax.axis_index("macro")
    rep = lax.axis_index("rep")
    local = rows * LANES
    amplitude = 1.0 / (reps * cells * STEPS * micro_dt)
    delta = fd_step * math.sqrt(macros * local)

    loads = [
        pltpu.make_async_copy(
            seed_ref.at[0, pl.ds(g * LANES, LANES), :], raw.at[g], load_sem.at[g]
        )
        for g in range(rows)
    ]
    for load in loads:
        load.start()

    barrier = pltpu.get_barrier_semaphore()
    for d in range(1, macros):
        pl.semaphore_signal(
            barrier, inc=1, device_id={"macro": lax.rem(me + d, macros)}, device_id_type=MESH
        )
    for d in range(1, reps):
        pl.semaphore_signal(
            barrier, inc=1, device_id={"rep": lax.rem(rep + d, reps)}, device_id_type=MESH
        )

    growth = micro_dt * rate_ref[...]
    scale = jnp.sqrt(growth)
    kappa = kappa_ref[...]
    coefs[5] = kappa
    coefs[6] = 1.0 + growth - 2.0 * kappa
    coefs[7] = 1.0 + growth
    unscale = 1.0 / scale
    coefs[8] = unscale
    coefs[9] = scale

    def row(index, g):
        return jnp.broadcast_to(coefs[index, pl.ds(g, 1), :], (SUB, LANES))

    for load in loads:
        load.wait()

    def prepare(g, carry):
        values = raw[g].astype(jnp.float32).T
        for s in range(SUB):
            flipped[s * pitch : s * pitch + depth, :] = values[s * depth : (s + 1) * depth]
        factor = row(9, g)
        acc = None
        for k in range(depth):
            kick = noise_amp * (flipped[pl.ds(k, SUB, stride=pitch), :] * seed_scale - 0.5)
            acc = kick if acc is None else acc + kick
            noise[g, k] = factor * kick
        noise_sum[pl.ds(g, 1), :] = jnp.sum(acc, axis=0, keepdims=True)
        return carry

    lax.fori_loop(0, rows, prepare, 0)

    pl.semaphore_wait(barrier, macros - 1 + reps - 1)

    lane = lax.broadcasted_iota(jnp.int32, (rows, LANES), 1)
    sub = lax.broadcasted_iota(jnp.int32, (SUB, LANES), 0)
    places = [(c + 0.5) / cells - 0.5 for c in range(cells)]
    square_sum = sum(x * x for x in places)
    first_place = sub.astype(jnp.float32) * (depth / cells) + (0.5 / cells - 0.5)
    edge = 0.5 + 0.5 / cells

    def send_whole(r, source, ds):
        copies = []
        for d in ds:
            copy = pltpu.make_async_remote_copy(
                src_ref=source,
                dst_ref=whole.at[r, d],
                send_sem=whole_send.at[r, d],
                recv_sem=whole_recv.at[r, d],
                device_id={"macro": lax.rem(me + (macros - d), macros)},
                device_id_type=MESH,
            )
            copy.start()
            copies.append(copy)
        return copies

    def send_parts(i):
        copies = []
        for d in range(1, reps):
            copy = pltpu.make_async_remote_copy(
                src_ref=parts.at[i, rep],
                dst_ref=parts.at[i, rep],
                send_sem=part_send.at[i, d],
                recv_sem=part_recv.at[i, d],
                device_id={"rep": lax.rem(rep + d, reps)},
                device_id_type=MESH,
            )
            copy.start()
            copies.append(copy)
        return copies

    def set_coefs(z, before, after):
        left_rows = jnp.concatenate([before, z[: rows - 1]], axis=0)
        right_rows = jnp.concatenate([z[1:], after], axis=0)
        left = jnp.where(lane == 0, pltpu.roll(left_rows, 1, 1), pltpu.roll(z, 1, 1))
        right = jnp.where(
            lane == LANES - 1,
            pltpu.roll(right_rows, LANES - 1, 1),
            pltpu.roll(z, LANES - 1, 1),
        )
        slope = 0.5 * (right - left)
        bend = 0.5 * (right - 2.0 * z + left)
        coefs[0] = scale * z
        coefs[1] = scale * slope
        coefs[2] = scale * bend
        coefs[3] = scale * (z - slope * edge + bend * edge * edge)
        coefs[4] = scale * (z + slope * edge + bend * edge * edge)
        return noise_sum[...] + cells * z + square_sum * bend

    def burst(i, g, unused):
        centre, slope, bend = row(0, g), row(1, g), row(2, g)
        ghost_left, ghost_right = row(3, g), row(4, g)
        kap, mid, top = row(5, g), row(6, g), row(7, g)
        base = centre + first_place * (slope + bend * first_place)
        tilt = slope + 2.0 * first_place * bend
        state = []
        for k in range(depth):
            shift = k / cells
            if k == 0:
                state.append(base + noise[g, k])
            else:
                state.append(base + shift * (tilt + shift * bend) + noise[g, k])
        for step in range(STEPS - 1):
            below = jnp.where(sub == 0, ghost_left, pltpu.roll(state[-1], 1, 0))
            above = jnp.where(sub == SUB - 1, ghost_right, pltpu.roll(state[0], SUB - 1, 0))
            padded = [below] + state + [above]
            state = [
                padded[k + 1] * (mid - padded[k + 1] * padded[k + 1])
                + kap * (padded[k] + padded[k + 2])
                for k in range(depth)
            ]
        sums = []
        for w in state:
            sums.append(w * (top - w * w))
        while len(sums) > 1:
            sums = [sums[t] + sums[t + 1] for t in range(0, len(sums), 2)]
        ends = jnp.where(sub == 0, ghost_left - state[0], 0.0) + jnp.where(
            sub == SUB - 1, ghost_right - state[-1], 0.0
        )
        grown = jnp.sum(sums[0] + kap * ends, axis=0, keepdims=True)
        parts[i, rep, pl.ds(g, 1), :] = grown * coefs[8, pl.ds(g, 1), :]
        return unused

    def bursts(i, indices):
        if len(indices) == 1:
            burst(i, indices[0], 0)
        else:
            stride = indices[1] - indices[0]
            lax.fori_loop(
                0, len(indices), lambda t, c: burst(i, indices[0] + t * stride, c), 0
            )

    def finish(i, start_sum, pending):
        parts[i, rep] = parts[i, rep] - start_sum
        copies = send_parts(i)
        for copy in pending:
            copy.wait_send()
        for copy in copies:
            copy.wait_recv()
        acc = parts[i, 0]
        for q in range(1, reps):
            acc = acc + parts[i, q]
        return acc * amplitude, copies

    has_left = me > 0
    has_right = me < macros - 1

    def outside(before, after):
        return (
            jnp.where(has_left, before, 0.0),
            jnp.where(has_right, after, 0.0),
        )

    def drift(i, z, before, after, pending):
        start_sum = set_coefs(z, *outside(before, after))
        bursts(i, list(range(rows)))
        return finish(i, start_sum, pending)

    sides = [1, macros - 1] if macros > 2 else [1]
    others = list(range(1, macros))

    def edges(r):
        return whole[r, macros - 1, rows - 1 : rows, :], whole[r, 1, 0:1, :]

    u_old = u_ref[...]
    old_copies = send_whole(0, u_ref, sides)
    nothing = jnp.zeros((1, LANES), jnp.float32)
    if rows > 2:
        set_coefs(u_old, nothing, nothing)
        bursts(0, list(range(1, rows - 1)))
    for copy in old_copies:
        copy.wait_recv()
    start_sum = set_coefs(u_old, *outside(*edges(0)))
    bursts(0, [0, rows - 1] if rows > 2 else list(range(rows)))
    f_old, sent_parts = finish(0, start_sum, old_copies)

    u_start = u_old + proj_step * f_old
    whole[1, 0] = u_start
    copies = send_whole(1, whole.at[1, 0], sides)
    for copy in sent_parts:
        copy.wait_send()
    for copy in copies:
        copy.wait_recv()
    u_before, u_after = edges(1)
    f_start, sent_parts = drift(1, u_start, u_before, u_after, copies)
    resid = -(u_start - u_old - proj_step * f_start)

    def gather(r, value, sent):
        whole[r, 0] = value
        copies = send_whole(r, whole.at[r, 0], others)
        for copy in sent:
            copy.wait_send()
        for copy in copies:
            copy.wait_recv()
        return whole[r].reshape(macros * rows, LANES), copies

    flat, copies = gather(2, resid, sent_parts)
    beta = jnp.sqrt(total(flat * flat))
    basis = [flat / beta]
    givens = Givens(beta)
    for j in range(ITERS):
        probe = basis[j]
        before = probe[macros * rows - 1 : macros * rows]
        after = probe[rows : rows + 1]
        f_probe, sent_parts = drift(
            j + 2,
            u_start + delta * probe[:rows],
            u_before + delta * before,
            u_after + delta * after,
            copies,
        )
        image = probe[:rows] - proj_step * (f_probe - f_start) / delta
        flat, copies = gather(j + 3, image, sent_parts)
        column = [total(vector * flat) for vector in basis]
        for coeff, vector in zip(column, basis):
            flat = flat - coeff * vector
        length = jnp.sqrt(total(flat * flat))
        column.append(length)
        givens.add(column)
        if j + 1 < ITERS:
            basis.append(flat / length)
    for copy in copies:
        copy.wait_send()
    result = u_start
    for coeff, vector in zip(givens.solve(), basis):
        result = result + coeff * vector[:rows]
    out_ref[...] = result


def solution(mesh):
    macros, reps = mesh.shape["macro"], mesh.shape["rep"]

    def step(u_old, rate, kappa, seed):
        local = u_old.shape[0]
        cells = seed.shape[2]
        rows = local // LANES
        depth = cells // SUB
        shape = (rows, LANES)
        vmem = pl.BlockSpec(memory_space=pltpu.VMEM)
        out = pl.pallas_call(
            functools.partial(kernel, macros, reps * seed.shape[0], cells, rows),
            out_shape=jax.ShapeDtypeStruct(shape, jnp.float32),
            in_specs=[vmem, vmem, vmem, pl.BlockSpec(memory_space=pl.ANY)],
            out_specs=vmem,
            scratch_shapes=[
                pltpu.VMEM((rows, LANES, cells), jnp.int32),
                pltpu.VMEM((SUB * (depth + 8), LANES), jnp.float32),
                pltpu.VMEM((rows, depth, SUB, LANES), jnp.float32),
                pltpu.VMEM(shape, jnp.float32),
                pltpu.VMEM((10,) + shape, jnp.float32),
                pltpu.VMEM((ITERS + 2, reps) + shape, jnp.float32),
                pltpu.VMEM((ITERS + 3, macros) + shape, jnp.float32),
                pltpu.SemaphoreType.DMA((rows,)),
                pltpu.SemaphoreType.DMA((ITERS + 2, reps)),
                pltpu.SemaphoreType.DMA((ITERS + 2, reps)),
                pltpu.SemaphoreType.DMA((ITERS + 3, macros)),
                pltpu.SemaphoreType.DMA((ITERS + 3, macros)),
            ],
            compiler_params=pltpu.CompilerParams(collective_id=0, has_side_effects=True),
        )(u_old.reshape(shape), rate.reshape(shape), kappa.reshape(shape), seed)
        return out.reshape(local)

    placed = (P("macro"), P("macro"), P("macro"), P("rep", "macro", None))
    return jax.shard_map(step, mesh=mesh, in_specs=placed, out_specs=P("macro"), check_vma=False)
```

```python
import functools
import math

import jax
import jax.numpy as jnp
from jax import lax
from jax.experimental import pallas as pl
from jax.experimental.pallas import tpu as pltpu
from jax.sharding import PartitionSpec as P

STEPS = 8
ITERS = 4
LANES = 128
SUB = 8

noise_amp = 1.0
micro_dt = 0.02
proj_step = 0.25
fd_step = 0.01
seed_scale = 2.0 ** (-30)

MESH = pl.DeviceIdType.MESH


def total(values):
    folded = jnp.sum(values, axis=0, keepdims=True)
    return jnp.sum(jnp.sum(folded, axis=1, keepdims=True), axis=2, keepdims=True)


class Givens:
    def __init__(self, beta):
        self.target = [beta]
        self.cosines = []
        self.sines = []
        self.upper = []

    def add(self, column):
        column = list(column)
        last = len(column) - 2
        for row in range(last):
            first, second = column[row], column[row + 1]
            column[row] = self.cosines[row] * first + self.sines[row] * second
            column[row + 1] = -self.sines[row] * first + self.cosines[row] * second
        radius = jnp.sqrt(column[last] * column[last] + column[last + 1] * column[last + 1])
        cosine = column[last] / radius
        sine = column[last + 1] / radius
        self.cosines.append(cosine)
        self.sines.append(sine)
        column[last] = radius
        self.upper.append(column[: last + 1])
        head = self.target[last]
        self.target[last] = cosine * head
        self.target.append(-sine * head)

    def solve(self):
        count = len(self.upper)
        solved = [None] * count
        for row in range(count - 1, -1, -1):
            acc = self.target[row]
            for later in range(row + 1, count):
                acc = acc - self.upper[later][row] * solved[later]
            solved[row] = acc / self.upper[row][row]
        return solved


def kernel(
    macros,
    reps,
    cells,
    rows,
    u_ref,
    rate_ref,
    kappa_ref,
    seed_ref,
    out_ref,
    raw,
    flipped,
    noise,
    noise_sum,
    coefs,
    parts,
    olds,
    load_sem,
    old_send,
    old_recv,
    part_send,
    part_recv,
):
    depth = cells // SUB
    pitch = flipped.shape[0] // SUB
    me = lax.axis_index("macro")
    rep = lax.axis_index("rep")
    local = rows * LANES
    amplitude = 1.0 / (reps * cells * STEPS * micro_dt)
    delta = fd_step * math.sqrt(macros * local)

    loads = [
        pltpu.make_async_copy(
            seed_ref.at[0, pl.ds(g * LANES, LANES), :], raw.at[g], load_sem.at[g]
        )
        for g in range(rows)
    ]
    for load in loads:
        load.start()

    barrier = pltpu.get_barrier_semaphore()
    peers = [(d, e) for d in range(macros) for e in range(reps)][1:]

    def peer(d, e):
        macro = me if d == 0 else lax.rem(me + (macros - d), macros)
        return {"macro": macro, "rep": rep if e == 0 else lax.rem(rep + e, reps)}

    for d, e in peers:
        pl.semaphore_signal(barrier, inc=1, device_id=peer(d, e), device_id_type=MESH)

    growth = micro_dt * rate_ref[...]
    scale = jnp.sqrt(growth)
    kappa = kappa_ref[...]
    coefs[5] = kappa
    coefs[6] = 1.0 + growth - 2.0 * kappa
    coefs[7] = 1.0 + growth
    unscale = 1.0 / scale
    coefs[8] = unscale
    coefs[9] = scale

    def row(index, g):
        return jnp.broadcast_to(coefs[index, pl.ds(g, 1), :], (SUB, LANES))

    for load in loads:
        load.wait()

    def prepare(g, carry):
        values = raw[g].astype(jnp.float32).T
        for s in range(SUB):
            flipped[s * pitch : s * pitch + depth, :] = values[s * depth : (s + 1) * depth]
        factor = row(9, g)
        acc = None
        for k in range(depth):
            kick = noise_amp * (flipped[pl.ds(k, SUB, stride=pitch), :] * seed_scale - 0.5)
            acc = kick if acc is None else acc + kick
            noise[g, k] = factor * kick
        noise_sum[pl.ds(g, 1), :] = jnp.sum(acc, axis=0, keepdims=True)
        return carry

    lax.fori_loop(0, rows, prepare, 0)

    pl.semaphore_wait(barrier, len(peers))

    lane = lax.broadcasted_iota(jnp.int32, (rows, LANES), 1)
    sub = lax.broadcasted_iota(jnp.int32, (SUB, LANES), 0)
    places = [(c + 0.5) / cells - 0.5 for c in range(cells)]
    square_sum = sum(x * x for x in places)
    first_place = sub.astype(jnp.float32) * (depth / cells) + (0.5 / cells - 0.5)
    edge = 0.5 + 0.5 / cells

    def send_parts(i):
        own = parts.at[i, rep]
        for d, e in peers:
            pltpu.make_async_remote_copy(
                src_ref=own,
                dst_ref=parts.at[i, d * reps + rep],
                send_sem=part_send.at[i],
                recv_sem=part_recv.at[i],
                device_id=peer(d, e),
                device_id_type=MESH,
            ).start()

    def all_sent(i):
        sent = parts.at[i, pl.ds(1, len(peers))]
        pltpu.make_async_copy(sent, sent, part_send.at[i]).wait()

    def all_received(i):
        got = parts.at[i, pl.ds(1, len(peers))]
        pltpu.make_async_copy(got, got, part_recv.at[i]).wait()

    def set_coefs(z, before, after):
        left_rows = jnp.concatenate([before, z[: rows - 1]], axis=0)
        right_rows = jnp.concatenate([z[1:], after], axis=0)
        left = jnp.where(lane == 0, pltpu.roll(left_rows, 1, 1), pltpu.roll(z, 1, 1))
        right = jnp.where(
            lane == LANES - 1,
            pltpu.roll(right_rows, LANES - 1, 1),
            pltpu.roll(z, LANES - 1, 1),
        )
        slope = 0.5 * (right - left)
        bend = 0.5 * (right - 2.0 * z + left)
        coefs[0] = scale * z
        coefs[1] = scale * slope
        coefs[2] = scale * bend
        coefs[3] = scale * (z - slope * edge + bend * edge * edge)
        coefs[4] = scale * (z + slope * edge + bend * edge * edge)
        coefs[10] = noise_sum[...] + cells * z + square_sum * bend

    def burst(i, g, unused):
        centre, slope, bend = row(0, g), row(1, g), row(2, g)
        ghost_left, ghost_right = row(3, g), row(4, g)
        kap, mid, top = row(5, g), row(6, g), row(7, g)
        base = centre + first_place * (slope + bend * first_place)
        tilt = slope + 2.0 * first_place * bend
        state = []
        for k in range(depth):
            shift = k / cells
            if k == 0:
                state.append(base + noise[g, k])
            else:
                state.append(base + shift * (tilt + shift * bend) + noise[g, k])
        for step in range(STEPS - 1):
            below = jnp.where(sub == 0, ghost_left, pltpu.roll(state[-1], 1, 0))
            above = jnp.where(sub == SUB - 1, ghost_right, pltpu.roll(state[0], SUB - 1, 0))
            padded = [below] + state + [above]
            state = [
                padded[k + 1] * (mid - padded[k + 1] * padded[k + 1])
                + kap * (padded[k] + padded[k + 2])
                for k in range(depth)
            ]
        sums = []
        for w in state:
            sums.append(w * (top - w * w))
        while len(sums) > 1:
            sums = [sums[t] + sums[t + 1] for t in range(0, len(sums), 2)]
        ends = jnp.where(sub == 0, ghost_left - state[0], 0.0) + jnp.where(
            sub == SUB - 1, ghost_right - state[-1], 0.0
        )
        grown = jnp.sum(sums[0] + kap * ends, axis=0, keepdims=True)
        change = grown * coefs[8, pl.ds(g, 1), :] - coefs[10, pl.ds(g, 1), :]
        parts[i, rep, pl.ds(g, 1), :] = change
        return unused

    def bursts(i, indices):
        if len(indices) == 1:
            burst(i, indices[0], 0)
        else:
            stride = indices[1] - indices[0]
            lax.fori_loop(
                0, len(indices), lambda t, c: burst(i, indices[0] + t * stride, c), 0
            )

    def finish(i):
        send_parts(i)
        if i:
            all_sent(i - 1)
        all_received(i)
        every = parts[i].reshape(macros, reps, rows, LANES)
        acc = every[:, 0]
        for q in range(1, reps):
            acc = acc + every[:, q]
        return acc * amplitude

    has_left = me > 0
    has_right = me < macros - 1

    def outside(before, after):
        return (
            jnp.where(has_left, before, 0.0),
            jnp.where(has_right, after, 0.0),
        )

    def edges(field):
        return field[macros - 1, rows - 1 : rows, :], field[1, 0:1, :]

    def drift(i, field):
        set_coefs(field[0], *outside(*edges(field)))
        bursts(i, list(range(rows)))
        return finish(i)

    copies = []
    for d in range(1, macros):
        copy = pltpu.make_async_remote_copy(
            src_ref=u_ref,
            dst_ref=olds.at[d],
            send_sem=old_send.at[d],
            recv_sem=old_recv.at[d],
            device_id=peer(d, 0),
            device_id_type=MESH,
        )
        copy.start()
        copies.append(copy)
    own = u_ref[...]
    olds[0] = own
    nothing = jnp.zeros((1, LANES), jnp.float32)
    if rows > 2:
        set_coefs(own, nothing, nothing)
        bursts(0, list(range(1, rows - 1)))
    for copy in copies:
        copy.wait()
    u_old = olds[...]
    set_coefs(own, *outside(*edges(u_old)))
    bursts(0, [0, rows - 1] if rows > 2 else list(range(rows)))
    f_old = finish(0)

    u_start = u_old + proj_step * f_old
    f_start = drift(1, u_start)
    resid = -(u_start - u_old - proj_step * f_start)
    beta = jnp.sqrt(total(resid * resid))
    basis = [resid / beta]
    givens = Givens(beta)
    for j in range(ITERS):
        probe = basis[j]
        f_probe = drift(j + 2, u_start + delta * probe)
        image = probe - proj_step * (f_probe - f_start) / delta
        column = [total(vector * image) for vector in basis]
        for coeff, vector in zip(column, basis):
            image = image - coeff * vector
        length = jnp.sqrt(total(image * image))
        column.append(length)
        givens.add(column)
        if j + 1 < ITERS:
            basis.append(image / length)
    all_sent(ITERS + 1)
    result = u_start[0]
    for coeff, vector in zip(givens.solve(), basis):
        result = result + coeff[0] * vector[0]
    out_ref[...] = result


def solution(mesh):
    macros, reps = mesh.shape["macro"], mesh.shape["rep"]

    def step(u_old, rate, kappa, seed):
        local = u_old.shape[0]
        cells = seed.shape[2]
        rows = local // LANES
        depth = cells // SUB
        shape = (rows, LANES)
        vmem = pl.BlockSpec(memory_space=pltpu.VMEM)
        out = pl.pallas_call(
            functools.partial(kernel, macros, reps * seed.shape[0], cells, rows),
            out_shape=jax.ShapeDtypeStruct(shape, jnp.float32),
            in_specs=[vmem, vmem, vmem, pl.BlockSpec(memory_space=pl.ANY)],
            out_specs=vmem,
            scratch_shapes=[
                pltpu.VMEM((rows, LANES, cells), jnp.int32),
                pltpu.VMEM((SUB * (depth + 8), LANES), jnp.float32),
                pltpu.VMEM((rows, depth, SUB, LANES), jnp.float32),
                pltpu.VMEM(shape, jnp.float32),
                pltpu.VMEM((11,) + shape, jnp.float32),
                pltpu.VMEM((ITERS + 2, macros * reps) + shape, jnp.float32),
                pltpu.VMEM((macros,) + shape, jnp.float32),
                pltpu.SemaphoreType.DMA((rows,)),
                pltpu.SemaphoreType.DMA((macros,)),
                pltpu.SemaphoreType.DMA((macros,)),
                pltpu.SemaphoreType.DMA((ITERS + 2,)),
                pltpu.SemaphoreType.DMA((ITERS + 2,)),
            ],
            compiler_params=pltpu.CompilerParams(collective_id=0, has_side_effects=True),
        )(u_old.reshape(shape), rate.reshape(shape), kappa.reshape(shape), seed)
        return out.reshape(local)

    placed = (P("macro"), P("macro"), P("macro"), P("rep", "macro", None))
    return jax.shard_map(step, mesh=mesh, in_specs=placed, out_specs=P("macro"), check_vma=False)
```

```python
import functools
import math

import jax
import jax.numpy as jnp
from jax import lax
from jax.experimental import pallas as pl
from jax.experimental.pallas import tpu as pltpu
from jax.sharding import PartitionSpec as P

STEPS = 8
ITERS = 4
LANES = 128
SUB = 8

noise_amp = 1.0
micro_dt = 0.02
proj_step = 0.25
fd_step = 0.01
seed_scale = 2.0 ** (-30)

MESH = pl.DeviceIdType.MESH


def total(values):
    folded = jnp.sum(values, axis=0, keepdims=True)
    return jnp.sum(jnp.sum(folded, axis=1, keepdims=True), axis=2, keepdims=True)


class Givens:
    def __init__(self, beta):
        self.target = [beta]
        self.cosines = []
        self.sines = []
        self.upper = []

    def add(self, column):
        column = list(column)
        last = len(column) - 2
        for row in range(last):
            first, second = column[row], column[row + 1]
            column[row] = self.cosines[row] * first + self.sines[row] * second
            column[row + 1] = -self.sines[row] * first + self.cosines[row] * second
        radius = jnp.sqrt(column[last] * column[last] + column[last + 1] * column[last + 1])
        cosine = column[last] / radius
        sine = column[last + 1] / radius
        self.cosines.append(cosine)
        self.sines.append(sine)
        column[last] = radius
        self.upper.append(column[: last + 1])
        head = self.target[last]
        self.target[last] = cosine * head
        self.target.append(-sine * head)

    def solve(self):
        count = len(self.upper)
        solved = [None] * count
        for row in range(count - 1, -1, -1):
            acc = self.target[row]
            for later in range(row + 1, count):
                acc = acc - self.upper[later][row] * solved[later]
            solved[row] = acc / self.upper[row][row]
        return solved


def kernel(
    macros,
    reps,
    cells,
    rows,
    u_in,
    rate_in,
    kappa_in,
    seed_ref,
    out_ref,
    u_ref,
    rate_ref,
    kappa_ref,
    edge_ref,
    raw,
    flipped,
    noise,
    noise_sum,
    coefs,
    parts,
    olds,
    load_sem,
    small_sem,
    old_send,
    old_recv,
    part_send,
    part_recv,
    near_recv,
):
    depth = cells // SUB
    pitch = flipped.shape[0] // SUB
    me = lax.axis_index("macro")
    rep = lax.axis_index("rep")
    local = rows * LANES
    amplitude = 1.0 / (reps * cells * STEPS * micro_dt)
    delta = fd_step * math.sqrt(macros * local)

    loads = [
        pltpu.make_async_copy(
            seed_ref.at[0, pl.ds(g * LANES, LANES), :], raw.at[g], load_sem.at[g]
        )
        for g in range(rows)
    ]
    small = [
        pltpu.make_async_copy(source, target, small_sem.at[t])
        for t, (source, target) in enumerate(
            [(rate_in, rate_ref), (kappa_in, kappa_ref), (u_in, u_ref)]
        )
    ]
    for load in small + loads:
        load.start()

    barrier = pltpu.get_barrier_semaphore()
    peers = [(d, e) for d in range(macros) for e in range(reps)][1:]

    def peer(d, e):
        macro = me if d == 0 else lax.rem(me + (macros - d), macros)
        return {"macro": macro, "rep": rep if e == 0 else lax.rem(rep + e, reps)}

    for d, e in peers:
        pl.semaphore_signal(barrier, inc=1, device_id=peer(d, e), device_id_type=MESH)

    for load in small:
        load.wait()
    growth = micro_dt * rate_ref[...]
    scale = jnp.sqrt(growth)
    kappa = kappa_ref[...]
    coefs[5] = kappa
    coefs[6] = 1.0 + growth - 2.0 * kappa
    coefs[7] = 1.0 + growth
    unscale = 1.0 / scale
    coefs[8] = unscale
    coefs[9] = scale

    def row(index, g):
        return jnp.broadcast_to(coefs[index, pl.ds(g, 1), :], (SUB, LANES))

    for load in loads:
        load.wait()

    def prepare(g, carry):
        values = raw[g].astype(jnp.float32).T
        for s in range(SUB):
            flipped[s * pitch : s * pitch + depth, :] = values[s * depth : (s + 1) * depth]
        factor = row(9, g)
        acc = None
        for k in range(depth):
            kick = noise_amp * (flipped[pl.ds(k, SUB, stride=pitch), :] * seed_scale - 0.5)
            acc = kick if acc is None else acc + kick
            noise[g, k] = factor * kick
        noise_sum[pl.ds(g, 1), :] = jnp.sum(acc, axis=0, keepdims=True)
        return carry

    lax.fori_loop(0, rows, prepare, 0)

    pl.semaphore_wait(barrier, len(peers))

    lane = lax.broadcasted_iota(jnp.int32, (rows, LANES), 1)
    sub = lax.broadcasted_iota(jnp.int32, (SUB, LANES), 0)
    places = [(c + 0.5) / cells - 0.5 for c in range(cells)]
    square_sum = sum(x * x for x in places)
    first_place = sub.astype(jnp.float32) * (depth / cells) + (0.5 / cells - 0.5)
    edge = 0.5 + 0.5 / cells

    near = {0: near_recv.at[0], 1: near_recv.at[1], macros - 1: near_recv.at[2]}

    def send_parts(i):
        own = parts.at[i, rep]
        for d, e in peers:
            pltpu.make_async_remote_copy(
                src_ref=own,
                dst_ref=parts.at[i, d * reps + rep],
                send_sem=part_send.at[i],
                recv_sem=part_recv.at[i] if i else near.get(d, part_recv.at[0]),
                device_id=peer(d, e),
                device_id_type=MESH,
            ).start()

    def all_sent(i):
        sent = parts.at[i, pl.ds(1, len(peers))]
        pltpu.make_async_copy(sent, sent, part_send.at[i]).wait()

    def near_received(d):
        got = parts.at[0, pl.ds(1, reps - 1) if d == 0 else pl.ds(d * reps, reps)]
        pltpu.make_async_copy(got, got, near[d]).wait()

    def far_received():
        got = parts.at[0, pl.ds(2 * reps, (macros - 3) * reps)]
        pltpu.make_async_copy(got, got, part_recv.at[0]).wait()

    def all_received(i):
        got = parts.at[i, pl.ds(1, len(peers))]
        pltpu.make_async_copy(got, got, part_recv.at[i]).wait()

    def set_coefs(z, before, after):
        left_rows = jnp.concatenate([before, z[: rows - 1]], axis=0)
        right_rows = jnp.concatenate([z[1:], after], axis=0)
        left = jnp.where(lane == 0, pltpu.roll(left_rows, 1, 1), pltpu.roll(z, 1, 1))
        right = jnp.where(
            lane == LANES - 1,
            pltpu.roll(right_rows, LANES - 1, 1),
            pltpu.roll(z, LANES - 1, 1),
        )
        slope = 0.5 * (right - left)
        bend = 0.5 * (right - 2.0 * z + left)
        coefs[0] = scale * z
        coefs[1] = scale * slope
        coefs[2] = scale * bend
        coefs[3] = scale * (z - slope * edge + bend * edge * edge)
        coefs[4] = scale * (z + slope * edge + bend * edge * edge)
        coefs[10] = noise_sum[...] + cells * z + square_sum * bend

    def burst(i, g, unused):
        centre, slope, bend = row(0, g), row(1, g), row(2, g)
        ghost_left, ghost_right = row(3, g), row(4, g)
        kap, mid, top = row(5, g), row(6, g), row(7, g)
        base = centre + first_place * (slope + bend * first_place)
        tilt = slope + 2.0 * first_place * bend
        state = []
        for k in range(depth):
            shift = k / cells
            if k == 0:
                state.append(base + noise[g, k])
            else:
                state.append(base + shift * (tilt + shift * bend) + noise[g, k])
        for step in range(STEPS - 1):
            below = jnp.where(sub == 0, ghost_left, pltpu.roll(state[-1], 1, 0))
            above = jnp.where(sub == SUB - 1, ghost_right, pltpu.roll(state[0], SUB - 1, 0))
            padded = [below] + state + [above]
            state = [
                padded[k + 1] * (mid - padded[k + 1] * padded[k + 1])
                + kap * (padded[k] + padded[k + 2])
                for k in range(depth)
            ]
        sums = []
        for w in state:
            sums.append(w * (top - w * w))
        while len(sums) > 1:
            sums = [sums[t] + sums[t + 1] for t in range(0, len(sums), 2)]
        ends = jnp.where(sub == 0, ghost_left - state[0], 0.0) + jnp.where(
            sub == SUB - 1, ghost_right - state[-1], 0.0
        )
        grown = jnp.sum(sums[0] + kap * ends, axis=0, keepdims=True)
        change = grown * coefs[8, pl.ds(g, 1), :] - coefs[10, pl.ds(g, 1), :]
        parts[i, rep, pl.ds(g, 1), :] = change
        return unused

    def bursts(i, indices):
        if len(indices) == 1:
            burst(i, indices[0], 0)
        else:
            stride = indices[1] - indices[0]
            lax.fori_loop(
                0, len(indices), lambda t, c: burst(i, indices[0] + t * stride, c), 0
            )

    def summed(i):
        every = parts[i].reshape(macros, reps, rows, LANES)
        acc = every[:, 0]
        for q in range(1, reps):
            acc = acc + every[:, q]
        return acc * amplitude

    def summed_block(d, first, last):
        acc = parts[0, d * reps, first:last, :]
        for q in range(1, reps):
            acc = acc + parts[0, d * reps + q, first:last, :]
        return acc * amplitude

    has_left = me > 0
    has_right = me < macros - 1

    def outside(before, after):
        return (
            jnp.where(has_left, before, 0.0),
            jnp.where(has_right, after, 0.0),
        )

    def edges(field):
        return field[macros - 1, rows - 1 : rows, :], field[1, 0:1, :]

    def drift(i, field):
        set_coefs(field[0], *outside(*edges(field)))
        bursts(i, list(range(rows)))
        send_parts(i)
        all_sent(i - 1)
        all_received(i)
        return summed(i)

    copies = []
    for d in range(1, macros):
        copy = pltpu.make_async_remote_copy(
            src_ref=u_ref,
            dst_ref=olds.at[d],
            send_sem=old_send.at[d],
            recv_sem=old_recv.at[d],
            device_id=peer(d, 0),
            device_id_type=MESH,
        )
        copy.start()
        copies.append(copy)
    own = u_ref[...]
    olds[0] = own
    nothing = jnp.zeros((1, LANES), jnp.float32)
    if rows > 2:
        set_coefs(own, nothing, nothing)
        bursts(0, list(range(1, rows - 1)))
    right_copy, left_copy = copies[0], copies[-1]
    edge_ref[...] = jnp.zeros_like(edge_ref)

    @pl.when(has_left)
    def _():
        left_copy.wait_recv()
        edge_ref[0] = olds[macros - 1, rows - 1 : rows, :]

    @pl.when(has_right)
    def _():
        right_copy.wait_recv()
        edge_ref[1] = olds[1, 0:1, :]

    set_coefs(own, edge_ref[0], edge_ref[1])
    bursts(0, [0, rows - 1] if rows > 2 else list(range(rows)))
    send_parts(0)
    near_received(0)

    @pl.when(has_left)
    def _():
        near_received(macros - 1)
        edge_ref[0] = edge_ref[0] + proj_step * summed_block(macros - 1, rows - 1, rows)

    @pl.when(has_right)
    def _():
        near_received(1)
        edge_ref[1] = edge_ref[1] + proj_step * summed_block(1, 0, 1)

    set_coefs(own + proj_step * summed_block(0, 0, rows), edge_ref[0], edge_ref[1])
    bursts(1, list(range(rows)))
    send_parts(1)

    @pl.when(jnp.logical_not(has_left))
    def _():
        left_copy.wait_recv()
        near_received(macros - 1)

    @pl.when(jnp.logical_not(has_right))
    def _():
        right_copy.wait_recv()
        near_received(1)

    for copy in copies[1:-1]:
        copy.wait_recv()
    for copy in copies:
        copy.wait_send()
    far_received()
    all_sent(0)
    u_old = olds[...]
    f_old = summed(0)
    u_start = u_old + proj_step * f_old
    all_received(1)
    f_start = summed(1)
    resid = -(u_start - u_old - proj_step * f_start)
    beta = jnp.sqrt(total(resid * resid))
    basis = [resid / beta]
    givens = Givens(beta)
    for j in range(ITERS):
        probe = basis[j]
        f_probe = drift(j + 2, u_start + delta * probe)
        image = probe - proj_step * (f_probe - f_start) / delta
        column = [total(vector * image) for vector in basis]
        for coeff, vector in zip(column, basis):
            image = image - coeff * vector
        length = jnp.sqrt(total(image * image))
        column.append(length)
        givens.add(column)
        if j + 1 < ITERS:
            basis.append(image / length)
    all_sent(ITERS + 1)
    result = u_start[0]
    for coeff, vector in zip(givens.solve(), basis):
        result = result + coeff[0] * vector[0]
    out_ref[...] = result


def solution(mesh):
    macros, reps = mesh.shape["macro"], mesh.shape["rep"]

    def step(u_old, rate, kappa, seed):
        local = u_old.shape[0]
        cells = seed.shape[2]
        rows = local // LANES
        depth = cells // SUB
        shape = (rows, LANES)
        vmem = pl.BlockSpec(memory_space=pltpu.VMEM)
        out = pl.pallas_call(
            functools.partial(kernel, macros, reps * seed.shape[0], cells, rows),
            out_shape=pltpu.VMEM(shape, jnp.float32),
            in_specs=[pl.BlockSpec(memory_space=pl.ANY)] * 4,
            out_specs=vmem,
            scratch_shapes=[
                pltpu.VMEM(shape, jnp.float32),
                pltpu.VMEM(shape, jnp.float32),
                pltpu.VMEM(shape, jnp.float32),
                pltpu.VMEM((2, 1, LANES), jnp.float32),
                pltpu.VMEM((rows, LANES, cells), jnp.int32),
                pltpu.VMEM((SUB * (depth + 8), LANES), jnp.float32),
                pltpu.VMEM((rows, depth, SUB, LANES), jnp.float32),
                pltpu.VMEM(shape, jnp.float32),
                pltpu.VMEM((11,) + shape, jnp.float32),
                pltpu.VMEM((ITERS + 2, macros * reps) + shape, jnp.float32),
                pltpu.VMEM((macros,) + shape, jnp.float32),
                pltpu.SemaphoreType.DMA((rows,)),
                pltpu.SemaphoreType.DMA((3,)),
                pltpu.SemaphoreType.DMA((macros,)),
                pltpu.SemaphoreType.DMA((macros,)),
                pltpu.SemaphoreType.DMA((ITERS + 2,)),
                pltpu.SemaphoreType.DMA((ITERS + 2,)),
                pltpu.SemaphoreType.DMA((3,)),
            ],
            compiler_params=pltpu.CompilerParams(collective_id=0, has_side_effects=True),
        )(u_old.reshape(shape), rate.reshape(shape), kappa.reshape(shape), seed)
        return out.reshape(local)

    placed = (P("macro"), P("macro"), P("macro"), P("rep", "macro", None))
    return jax.shard_map(step, mesh=mesh, in_specs=placed, out_specs=P("macro"), check_vma=False)
```

```python
import functools
import math

import jax
import jax.numpy as jnp
from jax import lax
from jax.experimental import pallas as pl
from jax.experimental.pallas import tpu as pltpu
from jax.sharding import PartitionSpec as P

STEPS = 8
ITERS = 4
LANES = 128
SUB = 8

noise_amp = 1.0
micro_dt = 0.02
proj_step = 0.25
fd_step = 0.01
seed_scale = 2.0 ** (-30)

MESH = pl.DeviceIdType.MESH


def total(values):
    folded = jnp.sum(values, axis=0, keepdims=True)
    return jnp.sum(jnp.sum(folded, axis=1, keepdims=True), axis=2, keepdims=True)


class Givens:
    def __init__(self, beta):
        self.target = [beta]
        self.cosines = []
        self.sines = []
        self.upper = []

    def add(self, column):
        column = list(column)
        last = len(column) - 2
        for row in range(last):
            first, second = column[row], column[row + 1]
            column[row] = self.cosines[row] * first + self.sines[row] * second
            column[row + 1] = -self.sines[row] * first + self.cosines[row] * second
        radius = jnp.sqrt(column[last] * column[last] + column[last + 1] * column[last + 1])
        cosine = column[last] / radius
        sine = column[last + 1] / radius
        self.cosines.append(cosine)
        self.sines.append(sine)
        column[last] = radius
        self.upper.append(column[: last + 1])
        head = self.target[last]
        self.target[last] = cosine * head
        self.target.append(-sine * head)

    def solve(self):
        count = len(self.upper)
        solved = [None] * count
        for row in range(count - 1, -1, -1):
            acc = self.target[row]
            for later in range(row + 1, count):
                acc = acc - self.upper[later][row] * solved[later]
            solved[row] = acc / self.upper[row][row]
        return solved


def kernel(
    macros,
    reps,
    cells,
    rows,
    u_in,
    rate_in,
    kappa_in,
    seed_ref,
    out_ref,
    u_ref,
    rate_ref,
    kappa_ref,
    edge_ref,
    raw,
    flipped,
    noise,
    noise_sum,
    coefs,
    parts,
    olds,
    load_sem,
    small_sem,
    old_send,
    old_recv,
    part_send,
    part_recv,
    near_recv,
):
    depth = cells // SUB
    pitch = flipped.shape[0] // SUB
    me = lax.axis_index("macro")
    rep = lax.axis_index("rep")
    local = rows * LANES
    amplitude = 1.0 / (reps * cells * STEPS * micro_dt)
    delta = fd_step * math.sqrt(macros * local)

    loads = [
        pltpu.make_async_copy(
            seed_ref.at[0, pl.ds(g * LANES, LANES), :], raw.at[g], load_sem.at[g]
        )
        for g in range(rows)
    ]
    small = [
        pltpu.make_async_copy(source, target, small_sem.at[t])
        for t, (source, target) in enumerate(
            [(rate_in, rate_ref), (kappa_in, kappa_ref), (u_in, u_ref)]
        )
    ]
    barrier = pltpu.get_barrier_semaphore()
    peers = [(d, e) for d in range(macros) for e in range(reps)][1:]

    def peer(d, e):
        macro = me if d == 0 else lax.rem(me + (macros - d), macros)
        return {"macro": macro, "rep": rep if e == 0 else lax.rem(rep + e, reps)}

    for d, e in peers:
        pl.semaphore_signal(barrier, inc=1, device_id=peer(d, e), device_id_type=MESH)

    for load in small + loads:
        load.start()
    for load in small:
        load.wait()
    growth = micro_dt * rate_ref[...]
    scale = jnp.sqrt(growth)
    kappa = kappa_ref[...]
    coefs[5] = kappa
    coefs[6] = 1.0 + growth - 2.0 * kappa
    coefs[7] = 1.0 + growth
    unscale = 1.0 / scale
    coefs[8] = unscale
    coefs[9] = scale

    def row(index, g):
        return jnp.broadcast_to(coefs[index, pl.ds(g, 1), :], (SUB, LANES))

    for load in loads:
        load.wait()

    def prepare(g, carry):
        values = raw[g].astype(jnp.float32).T
        for s in range(SUB):
            flipped[s * pitch : s * pitch + depth, :] = values[s * depth : (s + 1) * depth]
        factor = row(9, g)
        acc = None
        for k in range(depth):
            kick = noise_amp * (flipped[pl.ds(k, SUB, stride=pitch), :] * seed_scale - 0.5)
            acc = kick if acc is None else acc + kick
            noise[g, k] = factor * kick
        noise_sum[pl.ds(g, 1), :] = jnp.sum(acc, axis=0, keepdims=True)
        return carry

    lax.fori_loop(0, rows, prepare, 0)

    pl.semaphore_wait(barrier, len(peers))

    lane = lax.broadcasted_iota(jnp.int32, (rows, LANES), 1)
    sub = lax.broadcasted_iota(jnp.int32, (SUB, LANES), 0)
    places = [(c + 0.5) / cells - 0.5 for c in range(cells)]
    square_sum = sum(x * x for x in places)
    first_place = sub.astype(jnp.float32) * (depth / cells) + (0.5 / cells - 0.5)
    edge = 0.5 + 0.5 / cells

    near = {0: near_recv.at[0], 1: near_recv.at[1], macros - 1: near_recv.at[2]}

    far_first = sorted(peers, key=lambda p: (abs(p[1] - reps // 2), -(p[0] % 2), -abs(p[0] - macros / 2)))

    def send_parts(i):
        own = parts.at[i, rep]
        for d, e in far_first:
            pltpu.make_async_remote_copy(
                src_ref=own,
                dst_ref=parts.at[i, d * reps + rep],
                send_sem=part_send.at[i],
                recv_sem=part_recv.at[i] if i else near.get(d, part_recv.at[0]),
                device_id=peer(d, e),
                device_id_type=MESH,
            ).start()

    def all_sent(i):
        sent = parts.at[i, pl.ds(1, len(peers))]
        pltpu.make_async_copy(sent, sent, part_send.at[i]).wait()

    def near_received(d):
        got = parts.at[0, pl.ds(1, reps - 1) if d == 0 else pl.ds(d * reps, reps)]
        pltpu.make_async_copy(got, got, near[d]).wait()

    def far_received():
        got = parts.at[0, pl.ds(2 * reps, (macros - 3) * reps)]
        pltpu.make_async_copy(got, got, part_recv.at[0]).wait()

    def all_received(i):
        got = parts.at[i, pl.ds(1, len(peers))]
        pltpu.make_async_copy(got, got, part_recv.at[i]).wait()

    def set_coefs(z, before, after):
        left_rows = jnp.concatenate([before, z[: rows - 1]], axis=0)
        right_rows = jnp.concatenate([z[1:], after], axis=0)
        left = jnp.where(lane == 0, pltpu.roll(left_rows, 1, 1), pltpu.roll(z, 1, 1))
        right = jnp.where(
            lane == LANES - 1,
            pltpu.roll(right_rows, LANES - 1, 1),
            pltpu.roll(z, LANES - 1, 1),
        )
        slope = 0.5 * (right - left)
        bend = 0.5 * (right - 2.0 * z + left)
        coefs[0] = scale * z
        coefs[1] = scale * slope
        coefs[2] = scale * bend
        coefs[3] = scale * (z - slope * edge + bend * edge * edge)
        coefs[4] = scale * (z + slope * edge + bend * edge * edge)
        coefs[10] = noise_sum[...] + cells * z + square_sum * bend

    def burst(i, g, unused):
        centre, slope, bend = row(0, g), row(1, g), row(2, g)
        ghost_left, ghost_right = row(3, g), row(4, g)
        kap, mid, top = row(5, g), row(6, g), row(7, g)
        base = centre + first_place * (slope + bend * first_place)
        tilt = slope + 2.0 * first_place * bend
        state = []
        for k in range(depth):
            shift = k / cells
            if k == 0:
                state.append(base + noise[g, k])
            else:
                state.append(base + shift * (tilt + shift * bend) + noise[g, k])
        for step in range(STEPS - 1):
            below = jnp.where(sub == 0, ghost_left, pltpu.roll(state[-1], 1, 0))
            above = jnp.where(sub == SUB - 1, ghost_right, pltpu.roll(state[0], SUB - 1, 0))
            padded = [below] + state + [above]
            state = [
                padded[k + 1] * (mid - padded[k + 1] * padded[k + 1])
                + kap * (padded[k] + padded[k + 2])
                for k in range(depth)
            ]
        sums = []
        for w in state:
            sums.append(w * (top - w * w))
        while len(sums) > 1:
            sums = [sums[t] + sums[t + 1] for t in range(0, len(sums), 2)]
        ends = jnp.where(sub == 0, ghost_left - state[0], 0.0) + jnp.where(
            sub == SUB - 1, ghost_right - state[-1], 0.0
        )
        grown = jnp.sum(sums[0] + kap * ends, axis=0, keepdims=True)
        change = grown * coefs[8, pl.ds(g, 1), :] - coefs[10, pl.ds(g, 1), :]
        parts[i, rep, pl.ds(g, 1), :] = change
        return unused

    def bursts(i, indices):
        if len(indices) == 1:
            burst(i, indices[0], 0)
        else:
            stride = indices[1] - indices[0]
            lax.fori_loop(
                0, len(indices), lambda t, c: burst(i, indices[0] + t * stride, c), 0
            )

    def summed(i):
        every = parts[i].reshape(macros, reps, rows, LANES)
        acc = every[:, 0]
        for q in range(1, reps):
            acc = acc + every[:, q]
        return acc * amplitude

    def summed_block(d, first, last):
        acc = parts[0, d * reps, first:last, :]
        for q in range(1, reps):
            acc = acc + parts[0, d * reps + q, first:last, :]
        return acc * amplitude

    has_left = me > 0
    has_right = me < macros - 1

    def outside(before, after):
        return (
            jnp.where(has_left, before, 0.0),
            jnp.where(has_right, after, 0.0),
        )

    def edges(field):
        return field[macros - 1, rows - 1 : rows, :], field[1, 0:1, :]

    def drift(i, field):
        set_coefs(field[0], *outside(*edges(field)))
        bursts(i, list(range(rows)))
        send_parts(i)
        all_sent(i - 1)
        all_received(i)
        return summed(i)

    copies = []
    for d in range(1, macros):
        copy = pltpu.make_async_remote_copy(
            src_ref=u_ref,
            dst_ref=olds.at[d],
            send_sem=old_send.at[d],
            recv_sem=old_recv.at[d],
            device_id=peer(d, 0),
            device_id_type=MESH,
        )
        copy.start()
        copies.append(copy)
    own = u_ref[...]
    olds[0] = own
    nothing = jnp.zeros((1, LANES), jnp.float32)
    if rows > 2:
        set_coefs(own, nothing, nothing)
        bursts(0, list(range(1, rows - 1)))
    right_copy, left_copy = copies[0], copies[-1]
    edge_ref[...] = jnp.zeros_like(edge_ref)

    @pl.when(has_left)
    def _():
        left_copy.wait_recv()
        edge_ref[0] = olds[macros - 1, rows - 1 : rows, :]

    @pl.when(has_right)
    def _():
        right_copy.wait_recv()
        edge_ref[1] = olds[1, 0:1, :]

    set_coefs(own, edge_ref[0], edge_ref[1])
    bursts(0, [0, rows - 1] if rows > 2 else list(range(rows)))
    send_parts(0)
    near_received(0)

    @pl.when(has_left)
    def _():
        near_received(macros - 1)
        edge_ref[0] = edge_ref[0] + proj_step * summed_block(macros - 1, rows - 1, rows)

    @pl.when(has_right)
    def _():
        near_received(1)
        edge_ref[1] = edge_ref[1] + proj_step * summed_block(1, 0, 1)

    set_coefs(own + proj_step * summed_block(0, 0, rows), edge_ref[0], edge_ref[1])
    bursts(1, list(range(rows)))
    send_parts(1)

    @pl.when(jnp.logical_not(has_left))
    def _():
        left_copy.wait_recv()
        near_received(macros - 1)

    @pl.when(jnp.logical_not(has_right))
    def _():
        right_copy.wait_recv()
        near_received(1)

    for copy in copies[1:-1]:
        copy.wait_recv()
    for copy in copies:
        copy.wait_send()
    far_received()
    all_sent(0)
    u_old = olds[...]
    f_old = summed(0)
    u_start = u_old + proj_step * f_old
    all_received(1)
    f_start = summed(1)
    resid = -(u_start - u_old - proj_step * f_start)
    beta = jnp.sqrt(total(resid * resid))
    basis = [resid / beta]
    givens = Givens(beta)
    for j in range(ITERS):
        probe = basis[j]
        f_probe = drift(j + 2, u_start + delta * probe)
        image = probe - proj_step * (f_probe - f_start) / delta
        column = [total(vector * image) for vector in basis]
        for coeff, vector in zip(column, basis):
            image = image - coeff * vector
        length = jnp.sqrt(total(image * image))
        column.append(length)
        givens.add(column)
        if j + 1 < ITERS:
            basis.append(image / length)
    all_sent(ITERS + 1)
    result = u_start[0]
    for coeff, vector in zip(givens.solve(), basis):
        result = result + coeff[0] * vector[0]
    out_ref[...] = result


def solution(mesh):
    macros, reps = mesh.shape["macro"], mesh.shape["rep"]

    def step(u_old, rate, kappa, seed):
        local = u_old.shape[0]
        cells = seed.shape[2]
        rows = local // LANES
        depth = cells // SUB
        shape = (rows, LANES)
        vmem = pl.BlockSpec(memory_space=pltpu.VMEM)
        out = pl.pallas_call(
            functools.partial(kernel, macros, reps * seed.shape[0], cells, rows),
            out_shape=pltpu.VMEM(shape, jnp.float32),
            in_specs=[pl.BlockSpec(memory_space=pl.ANY)] * 4,
            out_specs=vmem,
            scratch_shapes=[
                pltpu.VMEM(shape, jnp.float32),
                pltpu.VMEM(shape, jnp.float32),
                pltpu.VMEM(shape, jnp.float32),
                pltpu.VMEM((2, 1, LANES), jnp.float32),
                pltpu.VMEM((rows, LANES, cells), jnp.int32),
                pltpu.VMEM((SUB * (depth + 8), LANES), jnp.float32),
                pltpu.VMEM((rows, depth, SUB, LANES), jnp.float32),
                pltpu.VMEM(shape, jnp.float32),
                pltpu.VMEM((11,) + shape, jnp.float32),
                pltpu.VMEM((ITERS + 2, macros * reps) + shape, jnp.float32),
                pltpu.VMEM((macros,) + shape, jnp.float32),
                pltpu.SemaphoreType.DMA((rows,)),
                pltpu.SemaphoreType.DMA((3,)),
                pltpu.SemaphoreType.DMA((macros,)),
                pltpu.SemaphoreType.DMA((macros,)),
                pltpu.SemaphoreType.DMA((ITERS + 2,)),
                pltpu.SemaphoreType.DMA((ITERS + 2,)),
                pltpu.SemaphoreType.DMA((3,)),
            ],
            compiler_params=pltpu.CompilerParams(collective_id=0, has_side_effects=True),
        )(u_old.reshape(shape), rate.reshape(shape), kappa.reshape(shape), seed)
        return out.reshape(local)

    placed = (P("macro"), P("macro"), P("macro"), P("rep", "macro", None))
    return jax.shard_map(step, mesh=mesh, in_specs=placed, out_specs=P("macro"), check_vma=False)
```
